8 devices in a mesh: dp: 1 (over z), a: 2 (over y), b: 4 (over x, core).
Axes of the slice: x: 2, y: 2, z: 1, core: 2. Of those that a mesh axis runs over, the one named last changes fastest.
Arguments:
- x: bfloat16 [2048, 8192], P('dp', ('a', 'b'))
- w_gate: bfloat16 [8192, 49152], P('a', 'b')
- w_up: bfloat16 [8192, 49152], P('a', 'b')
- w_down: bfloat16 [49152, 8192], P('b', 'a')
Outputs:
- output: bfloat16 [2048, 8192], P('dp', ('a', 'b'))
All inputs are finite; a program needn't handle non-finite values.
Results may differ from the reference program's by a relative error of at most 0.016.
Values are sent between devices in bfloat16 or wider.
A program may use at most 2 GiB of HBM per device.

```python
import jax
import jax.numpy as jnp

ROWS = 2048
D = 8192
FF = 49152


def setup_inputs(seed: int = 0, part: int = 0) -> dict:
    kx, kg, ku, kd = jax.random.split(jax.random.key(seed), 4)
    drawn = {
        "x": jax.random.normal(jax.random.fold_in(kx, part), (ROWS, D), jnp.float32),
        "w_gate": jax.random.normal(kg, (D, FF), jnp.float32) * D**-0.5,
        "w_up": jax.random.normal(ku, (D, FF), jnp.float32) * D**-0.5,
        "w_down": jax.random.normal(kd, (FF, D), jnp.float32) * FF**-0.5,
    }
    return {k: v.astype(jnp.bfloat16) for k, v in drawn.items()}


def reference(x, w_gate, w_up, w_down):
    gate = jnp.dot(x, w_gate, preferred_element_type=jnp.float32)
    up = jnp.dot(x, w_up, preferred_element_type=jnp.float32)
    hidden = (jax.nn.silu(gate) * up).astype(jnp.bfloat16)
    return jnp.dot(hidden, w_down, preferred_element_type=jnp.float32).astype(jnp.bfloat16)
```

```python
import jax
import jax.numpy as jnp
from jax import lax
from jax.sharding import PartitionSpec as P

CHUNKS = (256, 256, 256, 256)
PIECES = 4


def f32dot(l, r):
    return jnp.dot(l, r, preferred_element_type=jnp.float32)


def body(x, wg, wu, wd):
    bf16 = jnp.bfloat16
    a = lax.axis_index("a")
    ff = wg.shape[1]
    w = ff // PIECES
    swap = lambda v: lax.ppermute(v, "a", [(0, 1), (1, 0)])

    offs, o = [], 0
    for m in CHUNKS:
        offs.append(o)
        o += 2 * m

    def gathered(start, m):
        rows = lax.dynamic_slice_in_dim(x, start, m, 0)
        return lax.all_gather(rows, "b", axis=1, tiled=True)

    xs_other = [gathered(offs[c] + m * (1 - a), m) for c, m in enumerate(CHUNKS)]
    xs_own = [gathered(offs[c] + m * a, m) for c, m in enumerate(CHUNKS)]
    col = lambda v, p: lax.slice_in_dim(v, p * w, (p + 1) * w, axis=1)
    row = lambda v, p: lax.slice_in_dim(v, p * w, (p + 1) * w, axis=0)

    n = len(CHUNKS)
    got = {}

    def send_partials(c):
        for p in range(PIECES):
            with jax.named_scope(f"part_{c}_{p}"):
                g = f32dot(xs_other[c], col(wg, p)).astype(bf16)
                u = f32dot(xs_other[c], col(wu, p)).astype(bf16)
                got[c, p] = swap(g), swap(u)

    hid = {}
    out = jnp.zeros((x.shape[0], x.shape[1]), bf16)

    def own(c):
        for p in range(PIECES):
            with jax.named_scope(f"own_{c}_{p}"):
                rg, ru = got[c, p]
                g = f32dot(xs_own[c], col(wg, p)) + rg.astype(jnp.float32)
                u = f32dot(xs_own[c], col(wu, p)) + ru.astype(jnp.float32)
                h = (jax.nn.silu(g) * u).astype(bf16)
                hid[c, p] = h, swap(h)

    def down(c, out):
        m = CHUNKS[c]
        for side in range(2):
            with jax.named_scope(f"down_{c}_{side}"):
                y = None
                for p in range(PIECES):
                    t = f32dot(hid[c, p][side], row(wd, p))
                    y = t if y is None else y + t
                r = lax.psum_scatter(y.astype(bf16), "b", scatter_dimension=1, tiled=True)
                at = offs[c] + m * (a if side == 0 else 1 - a)
                out = lax.dynamic_update_slice_in_dim(out, r, at, 0)
        return out

    send_partials(0)
    for c in range(n):
        if c + 1 < n:
            send_partials(c + 1)
        own(c)
        out = down(c, out)
    return out


def solution(mesh):
    return jax.shard_map(
        body,
        mesh=mesh,
        in_specs=(P("dp", ("a", "b")), P("a", "b"), P("a", "b"), P("b", "a")),
        out_specs=P("dp", ("a", "b")),
        check_vma=False,
    )
```

```python
import functools

import jax
import jax.numpy as jnp
from jax import lax
from jax.experimental import pallas as pl
from jax.experimental.pallas import tpu as pltpu
from jax.sharding import PartitionSpec as P


HEAD = 128
HEAD_CUTS = (1024, 2048, 3072, 3072, 3072)
HEAD_GO = (3072, 3072, 2048, 2048, 1024, 1024)
BODY = (640, 256)
BODY_CUTS = (1024, 4352, 4352, 2560)
NB = 4

BF16, F32 = jnp.bfloat16, jnp.float32


MESH = pl.DeviceIdType.MESH


def places():
    me = lax.axis_index("b")
    return me, me + 1 - 2 * (me % 2), (me + 2) % NB


def greet(*others):
    barrier = pltpu.get_barrier_semaphore()
    for other in others:
        pl.semaphore_signal(barrier, inc=1, device_id={"b": other}, device_id_type=MESH)
    pl.semaphore_wait(barrier, len(others))


def remote(src, dst, send, recv, k, to):
    return pltpu.make_async_remote_copy(
        src_ref=src, dst_ref=dst, send_sem=send.at[k], recv_sem=recv.at[k],
        device_id={"b": to}, device_id_type=MESH,
    )


def block(i, cols):
    return pl.ds(pl.multiple_of(i * cols, cols), cols)


STEP = 256


def steps(n):
    return [slice(o, o + STEP) for o in range(0, n, STEP)]


def head_kernel(
    base, half, x_ref, wg_ref, wu_ref, g_ref, u_ref, o_ref, rb_ref, ro_ref,
    xs, ws, acc, stage, send, recv, local, wsem, ssem, tsem, osem,
):
    me, mate, far = places()
    order = (me, mate, far, (mate + 2) % NB)
    a = lax.axis_index("a")
    rows, cols, n = xs.shape[1], xs.shape[2], g_ref.shape[1]
    src = x_ref.at[pl.ds(pl.multiple_of(rows * (1 - a), rows), rows), :]
    own = pltpu.make_async_copy(src, xs.at[0], local)
    own.start()
    weights = []
    for i, blk in enumerate(order):
        at = pl.ds(pl.multiple_of(blk * cols, cols), cols)
        for j, w in enumerate((wg_ref, wu_ref)):
            k = 2 * i + j
            weights.append(pltpu.make_async_copy(w.at[at, pl.ds(0, n)], ws.at[k], wsem.at[k]))
    weights[0].start()
    weights[1].start()
    greet(mate, far)
    across = remote(src, xs.at[2], send, recv, 0, far)
    beside = remote(src, xs.at[1], send, recv, 1, mate)
    across.start()
    beside.start()
    for w in weights[2:]:
        w.start()
    pieces = (
        (base + half * (1 - a), rb_ref, 0, half),
        (rows * a, ro_ref, 0, rows),
        (base + half * a, ro_ref, rows, half),
    )
    ins, outs, o = [], [], 0
    for k, (at, dst, to, m) in enumerate(pieces):
        mid = stage.at[pl.ds(o, m), :]
        ins.append(
            pltpu.make_async_copy(x_ref.at[pl.ds(pl.multiple_of(at, rows), m), :], mid, ssem.at[k])
        )
        outs.append(pltpu.make_async_copy(mid, dst.at[pl.ds(to, m), :], tsem.at[k]))
        o += m
    for c in ins:
        c.start()

    def product(i):
        for j, o_bf in enumerate((g_ref, u_ref)):
            weights[2 * i + j].wait()
            for at in steps(n):
                t = jnp.dot(xs[i], ws[2 * i + j, :, at], preferred_element_type=F32)
                if i:
                    t = t + acc[j, :, at]
                if i < NB - 1:
                    acc[j, :, at] = t
                else:
                    o_bf[:, at] = t.astype(BF16)

    own.wait()
    product(0)
    beside.wait_recv()
    product(1)
    for c, d in zip(ins, outs):
        c.wait()
        d.start()
    across.wait_recv()
    relay = remote(xs.at[2], xs.at[3], send, recv, 2, mate)
    relay.start()
    product(2)
    relay.wait_recv()
    keeps = [
        pltpu.make_async_copy(xs.at[i], o_ref.at[:, block(blk, cols)], osem.at[i])
        for i, blk in enumerate(order)
    ]
    for c in keeps:
        c.start()
    product(3)
    for c in keeps + outs:
        c.wait()
    across.wait_send()
    beside.wait_send()
    relay.wait_send()


def gather_head(x, wg, wu, base, half, n):
    cols = x.shape[1]
    hbm, vmem = pl.BlockSpec(memory_space=pl.ANY), pl.BlockSpec(memory_space=pltpu.VMEM)
    shape = lambda *dims: jax.ShapeDtypeStruct(dims, BF16)
    dma = pltpu.SemaphoreType.DMA
    return pl.pallas_call(
        functools.partial(head_kernel, base, half),
        out_shape=(
            shape(HEAD, n), shape(HEAD, n), shape(HEAD, NB * cols),
            shape(half, cols), shape(HEAD + half, cols),
        ),
        in_specs=[hbm, hbm, hbm],
        out_specs=(vmem, vmem, hbm, hbm, hbm),
        scratch_shapes=[
            pltpu.VMEM((NB, HEAD, cols), BF16),
            pltpu.VMEM((2 * NB, cols, n), BF16),
            pltpu.VMEM((2, HEAD, n), F32),
            pltpu.VMEM((HEAD + 2 * half, cols), BF16),
            dma((3,)), dma((3,)), dma, dma((2 * NB,)), dma((3,)), dma((3,)), dma((NB,)),
        ],
        compiler_params=pltpu.CompilerParams(
            collective_id=0, has_side_effects=True, vmem_limit_bytes=60 << 20
        ),
        name="gather_head",
    )(x, wg, wu)


def tail_kernel(
    y_ref, h_ref, w_ref, o_ref, hb, ws, out, got, mid, send, recv, hsem, wsem
):
    me, mate, far = places()
    cols = o_ref.shape[1]
    depth = hb.shape[1]
    order = ((mate + 2) % NB, mate, far, me)
    here = pltpu.make_async_copy(h_ref, hb, hsem)
    here.start()
    weights = []
    for i, blk in enumerate(order):
        src = w_ref.at[pl.ds(w_ref.shape[0] - depth, depth), block(blk, cols)]
        weights.append(pltpu.make_async_copy(src, ws.at[i], wsem.at[i]))
        weights[-1].start()
    greet(mate, far)
    here.wait()

    def term(i, dst):
        weights[i].wait()
        for at in steps(cols):
            y = y_ref[:, pl.ds(pl.multiple_of(order[i] * cols + at.start, STEP), STEP)]
            y = y + jnp.dot(hb[...], ws[i, :, at], preferred_element_type=F32)
            dst[:, at] = y.astype(dst.dtype)

    first = [remote(out.at[k], got.at[k], send, recv, k, mate) for k in range(2)]
    for k in range(2):
        term(k, out.at[k])
        first[k].start()
    term(2, mid)
    first[0].wait_recv()
    out[2] = (mid[...] + got[0].astype(F32)).astype(BF16)
    last = remote(out.at[2], got.at[2], send, recv, 2, far)
    last.start()
    term(3, mid)
    first[1].wait_recv()
    last.wait_recv()
    o_ref[...] = (mid[...] + got[1].astype(F32) + got[2].astype(F32)).astype(BF16)
    for c in first:
        c.wait_send()
    last.wait_send()


def scatter_head(y, h, wd):
    rows, cols, depth = y.shape[0], y.shape[1] // NB, h.shape[1]
    hbm, vmem = pl.BlockSpec(memory_space=pl.ANY), pl.BlockSpec(memory_space=pltpu.VMEM)
    dma = pltpu.SemaphoreType.DMA
    return pl.pallas_call(
        tail_kernel,
        out_shape=jax.ShapeDtypeStruct((rows, cols), BF16),
        in_specs=[vmem, hbm, hbm],
        out_specs=vmem,
        scratch_shapes=[
            pltpu.VMEM((rows, depth), BF16),
            pltpu.VMEM((NB, depth, cols), BF16),
            pltpu.VMEM((3, rows, cols), BF16),
            pltpu.VMEM((3, rows, cols), BF16),
            pltpu.VMEM((rows, cols), F32),
            dma((3,)), dma((3,)), dma, dma((NB,)),
        ],
        compiler_params=pltpu.CompilerParams(
            collective_id=1, has_side_effects=True, vmem_limit_bytes=20 << 20
        ),
        name="scatter_head",
    )(y, h, wd)


def f32dot(l, r):
    return jnp.dot(l, r, preferred_element_type=F32)


def spans(cuts):
    out, o = [], 0
    for c in cuts:
        out.append((o, o + c))
        o += c
    return out


def body(x, wg, wu, wd):
    a, b = lax.axis_index("a"), lax.axis_index("b")
    cols = x.shape[1]
    half = x.shape[0] // 2 - HEAD
    swap = lambda v: lax.ppermute(v, "a", [(0, 1), (1, 0)])
    col = lambda v, s: lax.slice_in_dim(v, s[0], s[1], axis=1)
    row = lambda v, s: lax.slice_in_dim(v, s[0], s[1], axis=0)
    fence = lax.optimization_barrier
    nexts = [lax.rem(b + k, NB) * cols for k in range(NB)]

    def shift(v, k):
        return lax.ppermute(v, "b", [(i, (i + k) % NB) for i in range(NB)])

    def gather(rows):
        full = jnp.zeros((rows.shape[0], NB * cols), BF16)
        full = lax.dynamic_update_slice(full, rows, (0, nexts[0]))
        for k in (1, 2, 3):
            got = shift(rows, k)
            full = lax.dynamic_update_slice(full, got, (0, nexts[NB - k]))
        return full

    def scatter(y):
        total = lax.dynamic_slice_in_dim(y, nexts[0], cols, 1)
        for k in (1, 2, 3):
            out = lax.dynamic_slice_in_dim(y, nexts[k], cols, 1).astype(BF16)
            total = total + shift(out, k).astype(F32)
        return total.astype(BF16)

    base = 2 * HEAD
    head_spans, body_spans = spans(HEAD_CUTS), spans(BODY_CUTS)

    g0, u0, xh, body_rows, own_rows = gather_head(x, wg, wu, base, half, HEAD_CUTS[0])
    part = lambda xs, w, s: f32dot(xs, col(w, s)).astype(BF16)

    def swaps(g, u):
        return swap(g), swap(u)

    def parts(xs, s):
        g = part(xs, wg, s)
        return swaps(g, part(xs, wu, s))

    head_parts = [swaps(g0, u0)]
    head_parts += [parts(xh, s) for i, s in enumerate(head_spans) if i]
    x_other = gather(body_rows)
    x_own = gather(own_rows)
    body_parts = [parts(x_other, s) for s in body_spans]

    def hidden(xs, s, rg, ru):
        g = f32dot(xs, col(wg, s))
        u = f32dot(xs, col(wu, s)) + ru.astype(F32)
        return (jax.nn.silu(g + rg.astype(F32)) * u).astype(BF16)

    head_hid = [hidden(x_own[:HEAD], s, *head_parts[i]) for i, s in enumerate(head_spans)]
    head_hid = jnp.concatenate(lax.optimization_barrier(head_hid), 1)
    go_spans = spans(HEAD_GO)
    head_got = [swap(col(head_hid, s)) for s in go_spans]

    offs = spans(BODY)
    body_hid = [[] for _ in BODY]
    body_got = [[] for _ in BODY]
    for i, s in enumerate(body_spans):
        for j, o in enumerate(offs):
            xs = x_own[HEAD + o[0] : HEAD + o[1]]
            rg, ru = (row(v, o) for v in body_parts[i])
            h = hidden(xs, s, rg, ru)
            body_hid[j].append(h)
            body_got[j].append(swap(h))

    out = jnp.zeros((x.shape[0], cols), BF16)
    h = jnp.concatenate([head_hid] + [jnp.concatenate(v, 1) for v in body_hid])
    r = scatter(f32dot(h, wd))
    out = lax.dynamic_update_slice(out, r[:HEAD], (HEAD * a, 0))
    out = lax.dynamic_update_slice(out, r[HEAD:], (base + half * a, 0))

    def down(got, cuts, i):
        return f32dot(got[i], row(wd, cuts[i]))

    for j, o in enumerate(offs):
        n = len(body_spans)
        terms = fence([down(body_got[j], body_spans, i) for i in range(n - 1)])
        y = f32dot(body_got[j][-1], row(wd, body_spans[-1]))
        for t in terms:
            y = y + t
        at = base + half * (1 - a) + o[0]
        r = scatter(y)
        out = lax.dynamic_update_slice(out, r, (at, 0))

    y = down(head_got, go_spans, 0)
    for i in range(1, len(go_spans) - 1):
        y = fence(y) + down(head_got, go_spans, i)
    out, y = fence((out, y))
    r = scatter_head(y, head_got[-1], wd)
    return lax.dynamic_update_slice(out, r, (HEAD * (1 - a), 0))


def solution(mesh):
    return jax.shard_map(
        body,
        mesh=mesh,
        in_specs=(P("dp", ("a", "b")), P("a", "b"), P("a", "b"), P("b", "a")),
        out_specs=P("dp", ("a", "b")),
        check_vma=False,
    )
```

```python
import functools

import jax
import jax.numpy as jnp
from jax import lax
from jax.experimental import pallas as pl
from jax.experimental.pallas import tpu as pltpu
from jax.sharding import PartitionSpec as P


HEAD = 128
HEAD_CUTS = (1024, 2048, 2048, 3072, 4096)
HEAD_GO = (3072, 3072, 2048, 1792, 1280, 1024)
BODY = (640, 256)
BODY_CUTS = (1024, 4352, 4352, 2560)
NB = 4

BF16, F32 = jnp.bfloat16, jnp.float32


MESH = pl.DeviceIdType.MESH


def places():
    me = lax.axis_index("b")
    return me, me + 1 - 2 * (me % 2), (me + 2) % NB


def greet(*others):
    barrier = pltpu.get_barrier_semaphore()
    for other in others:
        pl.semaphore_signal(barrier, inc=1, device_id={"b": other}, device_id_type=MESH)
    pl.semaphore_wait(barrier, len(others))


def remote(src, dst, send, recv, k, to):
    return pltpu.make_async_remote_copy(
        src_ref=src, dst_ref=dst, send_sem=send.at[k], recv_sem=recv.at[k],
        device_id={"b": to}, device_id_type=MESH,
    )


def block(i, cols):
    return pl.ds(pl.multiple_of(i * cols, cols), cols)


STEP = 256


def steps(n):
    return [slice(o, o + STEP) for o in range(0, n, STEP)]


def head_kernel(
    base, half, x_ref, wg_ref, wu_ref, g_ref, u_ref, o_ref, rb_ref, ro_ref,
    xs, ws, acc, stage, send, recv, local, wsem, ssem, tsem, osem,
):
    me, mate, far = places()
    order = (me, mate, far, (mate + 2) % NB)
    a = lax.axis_index("a")
    rows, cols, n = xs.shape[1], xs.shape[2], g_ref.shape[1]
    src = x_ref.at[pl.ds(pl.multiple_of(rows * (1 - a), rows), rows), :]
    own = pltpu.make_async_copy(src, xs.at[0], local)
    own.start()
    weights = []
    for i, blk in enumerate(order):
        at = pl.ds(pl.multiple_of(blk * cols, cols), cols)
        for j, w in enumerate((wg_ref, wu_ref)):
            k = 2 * i + j
            weights.append(pltpu.make_async_copy(w.at[at, pl.ds(0, n)], ws.at[k], wsem.at[k]))
    weights[0].start()
    weights[1].start()
    greet(mate, far)
    across = remote(src, xs.at[2], send, recv, 0, far)
    beside = remote(src, xs.at[1], send, recv, 1, mate)
    across.start()
    beside.start()
    for w in weights[2:]:
        w.start()
    pieces = (
        (base + half * (1 - a), rb_ref, 0, half),
        (rows * a, ro_ref, 0, rows),
        (base + half * a, ro_ref, rows, half),
    )
    ins, outs, o = [], [], 0
    for k, (at, dst, to, m) in enumerate(pieces):
        mid = stage.at[pl.ds(o, m), :]
        ins.append(
            pltpu.make_async_copy(x_ref.at[pl.ds(pl.multiple_of(at, rows), m), :], mid, ssem.at[k])
        )
        outs.append(pltpu.make_async_copy(mid, dst.at[pl.ds(to, m), :], tsem.at[k]))
        o += m
    for c in ins:
        c.start()

    def product(i):
        for j, o_bf in enumerate((g_ref, u_ref)):
            weights[2 * i + j].wait()
            for at in steps(n):
                t = jnp.dot(xs[i], ws[2 * i + j, :, at], preferred_element_type=F32)
                if i:
                    t = t + acc[j, :, at]
                if i < NB - 1:
                    acc[j, :, at] = t
                else:
                    o_bf[:, at] = t.astype(BF16)

    own.wait()
    product(0)
    beside.wait_recv()
    product(1)
    for c, d in zip(ins, outs):
        c.wait()
        d.start()
    across.wait_recv()
    relay = remote(xs.at[2], xs.at[3], send, recv, 2, mate)
    relay.start()
    product(2)
    relay.wait_recv()
    keeps = [
        pltpu.make_async_copy(xs.at[i], o_ref.at[:, block(blk, cols)], osem.at[i])
        for i, blk in enumerate(order)
    ]
    for c in keeps:
        c.start()
    product(3)
    for c in keeps + outs:
        c.wait()
    across.wait_send()
    beside.wait_send()
    relay.wait_send()


def gather_head(x, wg, wu, base, half, n):
    cols = x.shape[1]
    hbm, vmem = pl.BlockSpec(memory_space=pl.ANY), pl.BlockSpec(memory_space=pltpu.VMEM)
    shape = lambda *dims: jax.ShapeDtypeStruct(dims, BF16)
    dma = pltpu.SemaphoreType.DMA
    return pl.pallas_call(
        functools.partial(head_kernel, base, half),
        out_shape=(
            shape(HEAD, n), shape(HEAD, n), shape(HEAD, NB * cols),
            shape(half, cols), shape(HEAD + half, cols),
        ),
        in_specs=[hbm, hbm, hbm],
        out_specs=(vmem, vmem, hbm, hbm, hbm),
        scratch_shapes=[
            pltpu.VMEM((NB, HEAD, cols), BF16),
            pltpu.VMEM((2 * NB, cols, n), BF16),
            pltpu.VMEM((2, HEAD, n), F32),
            pltpu.VMEM((HEAD + 2 * half, cols), BF16),
            dma((3,)), dma((3,)), dma, dma((2 * NB,)), dma((3,)), dma((3,)), dma((NB,)),
        ],
        compiler_params=pltpu.CompilerParams(
            collective_id=0, has_side_effects=True, vmem_limit_bytes=60 << 20
        ),
        name="gather_head",
    )(x, wg, wu)


def tail_kernel(
    y_ref, h_ref, w_ref, o_ref, hb, ws, out, got, mid, send, recv, hsem, wsem
):
    me, mate, far = places()
    cols = o_ref.shape[1]
    depth = hb.shape[1]
    order = ((mate + 2) % NB, far, mate, me)
    here = pltpu.make_async_copy(h_ref, hb, hsem)
    here.start()
    weights = []
    for i, blk in enumerate(order):
        src = w_ref.at[pl.ds(w_ref.shape[0] - depth, depth), block(blk, cols)]
        weights.append(pltpu.make_async_copy(src, ws.at[i], wsem.at[i]))
        weights[-1].start()
    greet(mate, far)
    here.wait()

    def term(i, dst):
        weights[i].wait()
        for at in steps(cols):
            y = y_ref[:, pl.ds(pl.multiple_of(order[i] * cols + at.start, STEP), STEP)]
            y = y + jnp.dot(hb[...], ws[i, :, at], preferred_element_type=F32)
            dst[:, at] = y.astype(dst.dtype)

    first = [remote(out.at[k], got.at[k], send, recv, k, mate) for k in range(2)]
    term(0, out.at[0])
    first[0].start()
    term(1, mid)
    first[0].wait_recv()
    out[2] = (mid[...] + got[0].astype(F32)).astype(BF16)
    last = remote(out.at[2], got.at[2], send, recv, 2, far)
    last.start()
    term(2, out.at[1])
    first[1].start()
    term(3, mid)
    first[1].wait_recv()
    last.wait_recv()
    o_ref[...] = (mid[...] + got[1].astype(F32) + got[2].astype(F32)).astype(BF16)
    for c in first:
        c.wait_send()
    last.wait_send()


def scatter_head(y, h, wd):
    rows, cols, depth = y.shape[0], y.shape[1] // NB, h.shape[1]
    hbm, vmem = pl.BlockSpec(memory_space=pl.ANY), pl.BlockSpec(memory_space=pltpu.VMEM)
    dma = pltpu.SemaphoreType.DMA
    return pl.pallas_call(
        tail_kernel,
        out_shape=jax.ShapeDtypeStruct((rows, cols), BF16),
        in_specs=[vmem, hbm, hbm],
        out_specs=vmem,
        scratch_shapes=[
            pltpu.VMEM((rows, depth), BF16),
            pltpu.VMEM((NB, depth, cols), BF16),
            pltpu.VMEM((3, rows, cols), BF16),
            pltpu.VMEM((3, rows, cols), BF16),
            pltpu.VMEM((rows, cols), F32),
            dma((3,)), dma((3,)), dma, dma((NB,)),
        ],
        compiler_params=pltpu.CompilerParams(
            collective_id=1, has_side_effects=True, vmem_limit_bytes=20 << 20
        ),
        name="scatter_head",
    )(y, h, wd)


def f32dot(l, r):
    return jnp.dot(l, r, preferred_element_type=F32)


def spans(cuts):
    out, o = [], 0
    for c in cuts:
        out.append((o, o + c))
        o += c
    return out


def body(x, wg, wu, wd):
    a, b = lax.axis_index("a"), lax.axis_index("b")
    cols = x.shape[1]
    half = x.shape[0] // 2 - HEAD
    swap = lambda v: lax.ppermute(v, "a", [(0, 1), (1, 0)])
    col = lambda v, s: lax.slice_in_dim(v, s[0], s[1], axis=1)
    row = lambda v, s: lax.slice_in_dim(v, s[0], s[1], axis=0)
    fence = lax.optimization_barrier
    nexts = [lax.rem(b + k, NB) * cols for k in range(NB)]

    def shift(v, k):
        return lax.ppermute(v, "b", [(i, (i + k) % NB) for i in range(NB)])

    def gather(rows):
        full = jnp.zeros((rows.shape[0], NB * cols), BF16)
        full = lax.dynamic_update_slice(full, rows, (0, nexts[0]))
        for k in (1, 2, 3):
            got = shift(rows, k)
            full = lax.dynamic_update_slice(full, got, (0, nexts[NB - k]))
        return full

    def scatter(y):
        total = lax.dynamic_slice_in_dim(y, nexts[0], cols, 1)
        for k in (1, 2, 3):
            out = lax.dynamic_slice_in_dim(y, nexts[k], cols, 1).astype(BF16)
            total = total + shift(out, k).astype(F32)
        return total.astype(BF16)

    base = 2 * HEAD
    head_spans, body_spans = spans(HEAD_CUTS), spans(BODY_CUTS)

    g0, u0, xh, body_rows, own_rows = gather_head(x, wg, wu, base, half, HEAD_CUTS[0])
    part = lambda xs, w, s: f32dot(xs, col(w, s)).astype(BF16)

    def swaps(g, u):
        return swap(g), swap(u)

    def parts(xs, s):
        g = part(xs, wg, s)
        return swaps(g, part(xs, wu, s))

    head_parts = [swaps(g0, u0)]
    head_parts += [parts(xh, s) for i, s in enumerate(head_spans) if i]
    x_other = gather(body_rows)
    x_own = gather(own_rows)
    body_parts = [parts(x_other, s) for s in body_spans[:-1]]
    g, u = (
        part(x_other, w, body_spans[-1])
        for w in (wg, wu)
    )
    u, head_parts = fence((u, head_parts))
    body_parts.append(swaps(g, u))

    def hidden(xs, s, rg, ru):
        g = f32dot(xs, col(wg, s))
        u = f32dot(xs, col(wu, s)) + ru.astype(F32)
        return (jax.nn.silu(g + rg.astype(F32)) * u).astype(BF16)

    received = fence([jnp.concatenate(v, 1) for v in zip(*head_parts)])
    head_hid = fence(hidden(x_own[:HEAD], (0, wg.shape[1]), *received))
    go_spans = spans(HEAD_GO)
    head_got = [swap(col(head_hid, s)) for s in go_spans]

    offs = spans(BODY)
    body_hid = []
    body_got = [[] for _ in BODY]
    for i, s in enumerate(body_spans):
        body_hid.append(fence(hidden(x_own[HEAD:], s, *body_parts[i])))
        for j, o in enumerate(offs):
            body_got[j].append(swap(row(body_hid[i], o)))

    out = jnp.zeros((x.shape[0], cols), BF16)
    h = jnp.concatenate([head_hid, jnp.concatenate(body_hid, 1)])
    r = scatter(f32dot(h, wd))
    out = lax.dynamic_update_slice(out, r[:HEAD], (HEAD * a, 0))
    out = lax.dynamic_update_slice(out, r[HEAD:], (base + half * a, 0))

    def down(got, cuts, i):
        return f32dot(got[i], row(wd, cuts[i]))

    for j, o in enumerate(offs):
        n = len(body_spans)
        terms = fence([down(body_got[j], body_spans, i) for i in range(n - 1)])
        y = f32dot(body_got[j][-1], row(wd, body_spans[-1]))
        for t in terms:
            y = y + t
        at = base + half * (1 - a) + o[0]
        r = scatter(y)
        out = lax.dynamic_update_slice(out, r, (at, 0))

    y = down(head_got, go_spans, 0)
    for i in range(1, len(go_spans) - 1):
        y = fence(y) + down(head_got, go_spans, i)
    out, y = fence((out, y))
    r = scatter_head(y, head_got[-1], wd)
    return lax.dynamic_update_slice(out, r, (HEAD * (1 - a), 0))


def solution(mesh):
    return jax.shard_map(
        body,
        mesh=mesh,
        in_specs=(P("dp", ("a", "b")), P("a", "b"), P("a", "b"), P("b", "a")),
        out_specs=P("dp", ("a", "b")),
        check_vma=False,
    )
```

```python
import functools

import jax
import jax.numpy as jnp
from jax import lax
from jax.experimental import pallas as pl
from jax.experimental.pallas import tpu as pltpu
from jax.sharding import PartitionSpec as P


HEAD = 128
HEAD_CUTS = (1024, 2048, 2048, 3072, 4096)
HEAD_GO = (3072, 3072, 2048, 1792, 1280, 1024)
BODY = (640, 256)
BODY_CUTS = (1024, 4352, 4352, 2560)
NB = 4

BF16, F32 = jnp.bfloat16, jnp.float32


MESH = pl.DeviceIdType.MESH


def places():
    me = lax.axis_index("b")
    return me, me + 1 - 2 * (me % 2), (me + 2) % NB


def greet(*others):
    barrier = pltpu.get_barrier_semaphore()
    for other in others:
        pl.semaphore_signal(barrier, inc=1, device_id={"b": other}, device_id_type=MESH)
    pl.semaphore_wait(barrier, len(others))


def remote(src, dst, send, recv, k, to):
    return pltpu.make_async_remote_copy(
        src_ref=src, dst_ref=dst, send_sem=send.at[k], recv_sem=recv.at[k],
        device_id={"b": to}, device_id_type=MESH,
    )


def block(i, cols):
    return pl.ds(pl.multiple_of(i * cols, cols), cols)


STEP = 256


def steps(n):
    return [slice(o, o + STEP) for o in range(0, n, STEP)]


def head_kernel(
    base, half, x_ref, wg_ref, wu_ref, g_ref, u_ref, o_ref, rb_ref, ro_ref,
    xs, ws, acc, stage, send, recv, local, wsem, ssem, tsem, osem,
):
    me, mate, far = places()
    order = (me, mate, far, (mate + 2) % NB)
    a = lax.axis_index("a")
    rows, cols, n = xs.shape[1], xs.shape[2], g_ref.shape[1]
    src = x_ref.at[pl.ds(pl.multiple_of(rows * (1 - a), rows), rows), :]
    own = pltpu.make_async_copy(src, xs.at[0], local)
    own.start()
    weights = []
    for i, blk in enumerate(order):
        at = pl.ds(pl.multiple_of(blk * cols, cols), cols)
        for j, w in enumerate((wg_ref, wu_ref)):
            k = 2 * i + j
            weights.append(pltpu.make_async_copy(w.at[at, pl.ds(0, n)], ws.at[k], wsem.at[k]))
    weights[0].start()
    weights[1].start()
    greet(mate, far)
    across = remote(src, xs.at[2], send, recv, 0, far)
    beside = remote(src, xs.at[1], send, recv, 1, mate)
    across.start()
    beside.start()
    for w in weights[2:]:
        w.start()
    pieces = (
        (base + half * (1 - a), rb_ref, 0, half),
        (rows * a, ro_ref, 0, rows),
        (base + half * a, ro_ref, rows, half),
    )
    ins, outs, o = [], [], 0
    for k, (at, dst, to, m) in enumerate(pieces):
        mid = stage.at[pl.ds(o, m), :]
        ins.append(
            pltpu.make_async_copy(x_ref.at[pl.ds(pl.multiple_of(at, rows), m), :], mid, ssem.at[k])
        )
        outs.append(pltpu.make_async_copy(mid, dst.at[pl.ds(to, m), :], tsem.at[k]))
        o += m
    for c in ins:
        c.start()

    def product(i):
        for j, o_bf in enumerate((g_ref, u_ref)):
            weights[2 * i + j].wait()
            for at in steps(n):
                t = jnp.dot(xs[i], ws[2 * i + j, :, at], preferred_element_type=F32)
                if i:
                    t = t + acc[j, :, at]
                if i < NB - 1:
                    acc[j, :, at] = t
                else:
                    o_bf[:, at] = t.astype(BF16)

    own.wait()
    product(0)
    beside.wait_recv()
    product(1)
    for c, d in zip(ins, outs):
        c.wait()
        d.start()
    across.wait_recv()
    relay = remote(xs.at[2], xs.at[3], send, recv, 2, mate)
    relay.start()
    product(2)
    relay.wait_recv()
    keeps = [
        pltpu.make_async_copy(xs.at[i], o_ref.at[:, block(blk, cols)], osem.at[i])
        for i, blk in enumerate(order)
    ]
    for c in keeps:
        c.start()
    product(3)
    for c in keeps + outs:
        c.wait()
    across.wait_send()
    beside.wait_send()
    relay.wait_send()


def gather_head(x, wg, wu, base, half, n):
    cols = x.shape[1]
    hbm, vmem = pl.BlockSpec(memory_space=pl.ANY), pl.BlockSpec(memory_space=pltpu.VMEM)
    shape = lambda *dims: jax.ShapeDtypeStruct(dims, BF16)
    dma = pltpu.SemaphoreType.DMA
    return pl.pallas_call(
        functools.partial(head_kernel, base, half),
        out_shape=(
            shape(HEAD, n), shape(HEAD, n), shape(HEAD, NB * cols),
            shape(half, cols), shape(HEAD + half, cols),
        ),
        in_specs=[hbm, hbm, hbm],
        out_specs=(vmem, vmem, hbm, hbm, hbm),
        scratch_shapes=[
            pltpu.VMEM((NB, HEAD, cols), BF16),
            pltpu.VMEM((2 * NB, cols, n), BF16),
            pltpu.VMEM((2, HEAD, n), F32),
            pltpu.VMEM((HEAD + 2 * half, cols), BF16),
            dma((3,)), dma((3,)), dma, dma((2 * NB,)), dma((3,)), dma((3,)), dma((NB,)),
        ],
        compiler_params=pltpu.CompilerParams(
            collective_id=0, has_side_effects=True, vmem_limit_bytes=60 << 20
        ),
        name="gather_head",
    )(x, wg, wu)


def tail_kernel(
    y_ref, h_ref, w_ref, o_ref, hb, ws, out, got, mid, send, recv, hsem, wsem
):
    me, mate, far = places()
    cols = o_ref.shape[1]
    depth = hb.shape[1]
    order = ((mate + 2) % NB, far, mate, me)
    here = pltpu.make_async_copy(h_ref, hb, hsem)
    here.start()
    weights = []
    for i, blk in enumerate(order):
        src = w_ref.at[pl.ds(w_ref.shape[0] - depth, depth), block(blk, cols)]
        weights.append(pltpu.make_async_copy(src, ws.at[i], wsem.at[i]))
        weights[-1].start()
    greet(mate, far)
    here.wait()

    def term(i, dst):
        weights[i].wait()
        for at in steps(cols):
            y = y_ref[:, pl.ds(pl.multiple_of(order[i] * cols + at.start, STEP), STEP)]
            y = y + jnp.dot(hb[...], ws[i, :, at], preferred_element_type=F32)
            dst[:, at] = y.astype(dst.dtype)

    first = [remote(out.at[k], got.at[k], send, recv, k, mate) for k in range(2)]
    term(0, out.at[0])
    first[0].start()
    term(1, mid)
    first[0].wait_recv()
    out[2] = (mid[...] + got[0].astype(F32)).astype(BF16)
    last = remote(out.at[2], got.at[2], send, recv, 2, far)
    last.start()
    term(2, out.at[1])
    first[1].start()
    term(3, mid)
    first[1].wait_recv()
    last.wait_recv()
    o_ref[...] = (mid[...] + got[1].astype(F32) + got[2].astype(F32)).astype(BF16)
    for c in first:
        c.wait_send()
    last.wait_send()


def scatter_head(y, h, wd):
    rows, cols, depth = y.shape[0], y.shape[1] // NB, h.shape[1]
    hbm, vmem = pl.BlockSpec(memory_space=pl.ANY), pl.BlockSpec(memory_space=pltpu.VMEM)
    dma = pltpu.SemaphoreType.DMA
    return pl.pallas_call(
        tail_kernel,
        out_shape=jax.ShapeDtypeStruct((rows, cols), BF16),
        in_specs=[vmem, hbm, hbm],
        out_specs=vmem,
        scratch_shapes=[
            pltpu.VMEM((rows, depth), BF16),
            pltpu.VMEM((NB, depth, cols), BF16),
            pltpu.VMEM((3, rows, cols), BF16),
            pltpu.VMEM((3, rows, cols), BF16),
            pltpu.VMEM((rows, cols), F32),
            dma((3,)), dma((3,)), dma, dma((NB,)),
        ],
        compiler_params=pltpu.CompilerParams(
            collective_id=1, has_side_effects=True, vmem_limit_bytes=20 << 20
        ),
        name="scatter_head",
    )(y, h, wd)


def f32dot(l, r):
    return jnp.dot(l, r, preferred_element_type=F32)


def spans(cuts):
    out, o = [], 0
    for c in cuts:
        out.append((o, o + c))
        o += c
    return out


def body(x, wg, wu, wd):
    a, b = lax.axis_index("a"), lax.axis_index("b")
    cols = x.shape[1]
    half = x.shape[0] // 2 - HEAD
    swap = lambda v: lax.ppermute(v, "a", [(0, 1), (1, 0)])
    col = lambda v, s: lax.slice_in_dim(v, s[0], s[1], axis=1)
    row = lambda v, s: lax.slice_in_dim(v, s[0], s[1], axis=0)
    fence = lax.optimization_barrier
    nexts = [lax.rem(b + k, NB) * cols for k in range(NB)]

    def shift(v, k):
        return lax.ppermute(v, "b", [(i, (i + k) % NB) for i in range(NB)])

    def gather(rows):
        full = jnp.zeros((rows.shape[0], NB * cols), BF16)
        full = lax.dynamic_update_slice(full, rows, (0, nexts[0]))
        for k in (1, 2, 3):
            got = shift(rows, k)
            full = lax.dynamic_update_slice(full, got, (0, nexts[NB - k]))
        return full

    def scatter(y):
        total = lax.dynamic_slice_in_dim(y, nexts[0], cols, 1)
        for k in (1, 2, 3):
            out = lax.dynamic_slice_in_dim(y, nexts[k], cols, 1).astype(BF16)
            total = total + shift(out, k).astype(F32)
        return total.astype(BF16)

    base = 2 * HEAD
    head_spans, body_spans = spans(HEAD_CUTS), spans(BODY_CUTS)

    g0, u0, xh, body_rows, own_rows = gather_head(x, wg, wu, base, half, HEAD_CUTS[0])
    part = lambda xs, w, s: f32dot(xs, col(w, s)).astype(BF16)

    def swaps(g, u):
        return swap(g), swap(u)

    def parts(xs, s):
        g = part(xs, wg, s)
        return swaps(g, part(xs, wu, s))

    head_parts = [swaps(g0, u0)]
    head_parts += [parts(xh, s) for i, s in enumerate(head_spans) if i]
    x_other = gather(body_rows)
    x_own = gather(own_rows)
    body_parts = [parts(x_other, s) for s in body_spans]

    def hidden(xs, s, rg, ru):
        g = f32dot(xs, col(wg, s))
        u = f32dot(xs, col(wu, s)) + ru.astype(F32)
        return (jax.nn.silu(g + rg.astype(F32)) * u).astype(BF16)

    head_hid = [hidden(x_own[:HEAD], s, *head_parts[i]) for i, s in enumerate(head_spans)]
    head_hid = jnp.concatenate(lax.optimization_barrier(head_hid), 1)
    go_spans = spans(HEAD_GO)
    head_got = [swap(col(head_hid, s)) for s in go_spans]

    offs = spans(BODY)
    body_hid = [[] for _ in BODY]
    body_got = [[] for _ in BODY]
    for i, s in enumerate(body_spans):
        for j, o in enumerate(offs):
            xs = x_own[HEAD + o[0] : HEAD + o[1]]
            rg, ru = (row(v, o) for v in body_parts[i])
            h = hidden(xs, s, rg, ru)
            body_hid[j].append(h)
            body_got[j].append(swap(h))

    out = jnp.zeros((x.shape[0], cols), BF16)
    h = jnp.concatenate([head_hid] + [jnp.concatenate(v, 1) for v in body_hid])
    r = scatter(f32dot(h, wd))
    out = lax.dynamic_update_slice(out, r[:HEAD], (HEAD * a, 0))
    out = lax.dynamic_update_slice(out, r[HEAD:], (base + half * a, 0))

    def down(got, cuts, i):
        return f32dot(got[i], row(wd, cuts[i]))

    for j, o in enumerate(offs):
        n = len(body_spans)
        terms = fence([down(body_got[j], body_spans, i) for i in range(n - 1)])
        y = f32dot(body_got[j][-1], row(wd, body_spans[-1]))
        for t in terms:
            y = y + t
        at = base + half * (1 - a) + o[0]
        r = scatter(y)
        out = lax.dynamic_update_slice(out, r, (at, 0))

    y = down(head_got, go_spans, 0)
    for i in range(1, len(go_spans) - 1):
        y = fence(y) + down(head_got, go_spans, i)
    out, y = fence((out, y))
    r = scatter_head(y, head_got[-1], wd)
    return lax.dynamic_update_slice(out, r, (HEAD * (1 - a), 0))


def solution(mesh):
    return jax.shard_map(
        body,
        mesh=mesh,
        in_specs=(P("dp", ("a", "b")), P("a", "b"), P("a", "b"), P("b", "a")),
        out_specs=P("dp", ("a", "b")),
        check_vma=False,
    )
```
